8 devices in a mesh: dp: 1 (over z), tp: 8 (over y, x, core).
Axes of the slice: x: 2, y: 2, z: 1, core: 2. Of those that a mesh axis runs over, the one named last changes fastest.
Arguments:
- hidden: bfloat16 [6, 768, 4096], P('dp', 'tp')
- grad_out: bfloat16 [6, 768, 4096], P('dp', 'tp')
- prefix_len: int32 [6], P('dp')
- valid_len: int32 [6], P('dp')
- attn_norm: bfloat16 [4096], replicated
- w_query: bfloat16 [4096, 4096], P(None, 'tp')
- w_key: bfloat16 [4096, 256], replicated
- w_value: bfloat16 [4096, 256], replicated
- w_out: bfloat16 [4096, 4096], P('tp')
- mlp_norm: bfloat16 [4096], replicated
- w_gate: bfloat16 [4096, 16384], P(None, 'tp')
- w_up: bfloat16 [4096, 16384], P(None, 'tp')
- w_down: bfloat16 [16384, 4096], P('tp')
Outputs:
- output 1: bfloat16 [6, 768, 4096], P('dp', 'tp')
- output 2: bfloat16 [6, 768, 4096], P('dp', 'tp')
- output 3: float32 [4096], P('dp')
- output 4: float32 [4096, 4096], P('dp', 'tp')
- output 5: float32 [4096, 256], P('dp')
- output 6: float32 [4096, 256], P('dp')
- output 7: float32 [4096, 4096], P(('dp', 'tp'))
- output 8: float32 [4096], P('dp')
- output 9: float32 [4096, 16384], P('dp', 'tp')
- output 10: float32 [4096, 16384], P('dp', 'tp')
- output 11: float32 [16384, 4096], P(('dp', 'tp'))
All inputs are finite; a program needn't handle non-finite values.
Results may differ from the reference program's by a relative error of at most 0.02.
Values are sent between devices in bfloat16 or wider.
A program may use at most 1 GiB of HBM per device.

```python
import math
import jax
import jax.numpy as jnp
from jax import lax

BATCH_SIZE = 6
SEQ_LEN = 768
MODEL_DIM = 4096
NUM_HEADS = 16
HEAD_DIM = 256
FFN_DIM = 16384


def rms_norm(x_in, gain):
    x_f = x_in.astype(jnp.float32)
    inv_rms = lax.rsqrt(jnp.mean(x_f * x_f, axis=-1, keepdims=True) + 1e-6)
    return (x_f * inv_rms * (1.0 + gain.astype(jnp.float32))).astype(jnp.bfloat16)


def rope_tables(positions, head_dim):
    half_dim = head_dim // 2
    exponent = jnp.arange(half_dim, dtype=jnp.float32) * (2.0 / head_dim)
    inv_freq = jnp.exp(exponent * (-math.log(10000.0)))
    angles = positions.astype(jnp.float32)[:, None] * inv_freq[None, :]
    return jnp.cos(angles), jnp.sin(angles)


def apply_rope(x_f, cos_t, sin_t):
    half_dim = x_f.shape[-1] // 2
    first = x_f[..., :half_dim]
    second = x_f[..., half_dim:]
    return jnp.concatenate([first * cos_t - second * sin_t, second * cos_t + first * sin_t], axis=-1)


def attend_one(operands):
    query, keys, values, prefix_count, valid_count = operands
    seq_len = query.shape[0]
    scale = query.shape[-1] ** -0.5
    scores = jnp.einsum("qhd,kd->hqk", query.astype(jnp.float32), keys.astype(jnp.float32)) * scale
    q_pos = jnp.arange(seq_len)[:, None]
    k_pos = jnp.arange(seq_len)[None, :]
    visible = (k_pos < valid_count) & ((k_pos < prefix_count) | (k_pos <= q_pos))
    scores = jnp.where(visible[None], scores, -1e30)
    probs = jax.nn.softmax(scores, axis=-1).astype(jnp.bfloat16)
    mixed = jnp.einsum("hqk,kd->qhd", probs.astype(jnp.float32), values.astype(jnp.float32))
    return mixed.astype(jnp.bfloat16)


def layer_forward(hidden, prefix_len, valid_len, weights):
    attn_norm, w_query, w_key, w_value, w_out, mlp_norm, w_gate, w_up, w_down = weights
    batch, seq_len, model_dim = hidden.shape
    head_dim = w_key.shape[1]
    num_heads = w_query.shape[1] // head_dim
    num_rows = batch * seq_len
    normed = rms_norm(hidden, attn_norm).reshape(num_rows, model_dim)
    cos_t, sin_t = rope_tables(jnp.arange(seq_len), head_dim)
    q_raw = jnp.dot(normed, w_query, preferred_element_type=jnp.float32).reshape(batch, seq_len, num_heads, head_dim)
    query = apply_rope(q_raw, cos_t[:, None, :], sin_t[:, None, :]).astype(jnp.bfloat16)
    k_raw = jnp.dot(normed, w_key, preferred_element_type=jnp.float32).reshape(batch, seq_len, head_dim)
    keys = apply_rope(k_raw, cos_t, sin_t).astype(jnp.bfloat16)
    values = jnp.dot(normed, w_value, preferred_element_type=jnp.float32).astype(jnp.bfloat16).reshape(batch, seq_len, head_dim)
    mixed = lax.map(jax.checkpoint(attend_one), (query, keys, values, prefix_len, valid_len))
    attn_out = jnp.dot(mixed.reshape(num_rows, num_heads * head_dim), w_out, preferred_element_type=jnp.float32)
    resid = (hidden.astype(jnp.float32) + attn_out.reshape(batch, seq_len, model_dim)).astype(jnp.bfloat16)
    gated_in = rms_norm(resid, mlp_norm).reshape(num_rows, model_dim)
    gate = jnp.dot(gated_in, w_gate, preferred_element_type=jnp.float32)
    upper = jnp.dot(gated_in, w_up, preferred_element_type=jnp.float32)
    act = (jax.nn.gelu(gate, approximate=True) * upper).astype(jnp.bfloat16)
    mlp_out = jnp.dot(act, w_down, preferred_element_type=jnp.float32)
    return (resid.astype(jnp.float32) + mlp_out.reshape(batch, seq_len, model_dim)).astype(jnp.bfloat16)


def setup_inputs(seed: int = 0, part: int = 0) -> dict:
    base_key = jax.random.key(seed)
    part_keys = jax.random.split(jax.random.fold_in(base_key, part), 4)
    shared_keys = jax.random.split(base_key, 9)
    q_dim = NUM_HEADS * HEAD_DIM
    act_shape = (BATCH_SIZE, SEQ_LEN, MODEL_DIM)
    hidden = (0.25 * jax.random.normal(part_keys[0], act_shape, jnp.float32)).astype(jnp.bfloat16)
    grad_out = jax.random.normal(part_keys[1], act_shape, jnp.float32).astype(jnp.bfloat16)
    valid_len = jax.random.randint(part_keys[2], (BATCH_SIZE,), (3 * SEQ_LEN) // 4, SEQ_LEN + 1, dtype=jnp.int32)
    valid_len = valid_len.at[0].set(SEQ_LEN)
    prefix_len = jax.random.randint(part_keys[3], (BATCH_SIZE,), SEQ_LEN // 8, (3 * SEQ_LEN) // 4 + 1, dtype=jnp.int32)
    in_scale = 1.0 / math.sqrt(MODEL_DIM)
    out_scale = math.sqrt(SEQ_LEN / (64.0 * q_dim))
    down_scale = 1.0 / math.sqrt(FFN_DIM)
    attn_norm = (0.3 * jax.random.normal(shared_keys[0], (MODEL_DIM,), jnp.float32)).astype(jnp.bfloat16)
    w_query = (in_scale * jax.random.normal(shared_keys[1], (MODEL_DIM, q_dim), jnp.float32)).astype(jnp.bfloat16)
    w_key = (in_scale * jax.random.normal(shared_keys[2], (MODEL_DIM, HEAD_DIM), jnp.float32)).astype(jnp.bfloat16)
    w_value = (in_scale * jax.random.normal(shared_keys[3], (MODEL_DIM, HEAD_DIM), jnp.float32)).astype(jnp.bfloat16)
    w_out = (out_scale * jax.random.normal(shared_keys[4], (q_dim, MODEL_DIM), jnp.float32)).astype(jnp.bfloat16)
    mlp_norm = (0.3 * jax.random.normal(shared_keys[5], (MODEL_DIM,), jnp.float32)).astype(jnp.bfloat16)
    w_gate = (in_scale * jax.random.normal(shared_keys[6], (MODEL_DIM, FFN_DIM), jnp.float32)).astype(jnp.bfloat16)
    w_up = (in_scale * jax.random.normal(shared_keys[7], (MODEL_DIM, FFN_DIM), jnp.float32)).astype(jnp.bfloat16)
    w_down = (down_scale * jax.random.normal(shared_keys[8], (FFN_DIM, MODEL_DIM), jnp.float32)).astype(jnp.bfloat16)
    return {"hidden": hidden, "grad_out": grad_out, "prefix_len": prefix_len, "valid_len": valid_len, "attn_norm": attn_norm, "w_query": w_query, "w_key": w_key, "w_value": w_value, "w_out": w_out, "mlp_norm": mlp_norm, "w_gate": w_gate, "w_up": w_up, "w_down": w_down}


def reference(hidden, grad_out, prefix_len, valid_len, attn_norm, w_query, w_key, w_value, w_out, mlp_norm, w_gate, w_up, w_down):
    weights = (attn_norm, w_query, w_key, w_value, w_out, mlp_norm, w_gate, w_up, w_down)

    def forward(hidden_in, weights_in):
        return layer_forward(hidden_in, prefix_len, valid_len, weights_in)

    hidden_out, pullback = jax.vjp(forward, hidden, weights)
    grad_hidden, grad_weights = pullback(grad_out)
    g_attn_norm, g_query, g_key, g_value, g_out, g_mlp_norm, g_gate, g_up, g_down = grad_weights
    return (hidden_out, grad_hidden, g_attn_norm.astype(jnp.float32), g_query.astype(jnp.float32), g_key.astype(jnp.float32), g_value.astype(jnp.float32), g_out.astype(jnp.float32), g_mlp_norm.astype(jnp.float32), g_gate.astype(jnp.float32), g_up.astype(jnp.float32), g_down.astype(jnp.float32))
```

```python
import math
import functools
import jax
import jax.numpy as jnp
from jax import lax
from jax.experimental import pallas as pl
from jax.experimental.pallas import tpu as pltpu
from jax.sharding import PartitionSpec as P

NORM_EPS = 1e-6
NUM_CHUNKS = 2
F32 = jnp.float32
BF16 = jnp.bfloat16


def swap(x, mask):
    return lax.ppermute(x, "tp", [(i, i ^ mask) for i in range(8)])


class Order:
    def __init__(self):
        self.last = None

    def tie(self, *xs):
        if self.last is None:
            return xs
        return lax.optimization_barrier((*xs, self.last))[:-1]

    def step(self, fn, *xs):
        out = fn(*self.tie(*xs))
        self.last = jax.tree.leaves(out)[0]
        return out


class Gather:
    def __init__(self, order, x):
        self.order, self.x = order, x
        half = x.shape[0] // 2
        (x,) = order.tie(x)
        top, bottom = x[:half], x[half:]
        self.p2a, self.p4b = swap(top, 2), swap(bottom, 4)
        self.p2b, self.p4a = swap(bottom, 2), swap(top, 4)

    def forward(self):
        self.p2a, self.p4b = self.order.tie(self.p2a, self.p4b)
        self.order.last = self.p2a
        self.s6a, self.s6b = swap(self.p2a, 4), swap(self.p4b, 2)

    def finish(self):
        parts = (self.x, self.p2a, self.p2b, self.p4a, self.p4b, self.s6a, self.s6b)
        even = self.order.step(lambda *p: jnp.concatenate(p, axis=0), *parts)
        return even, swap(even, 1)


class Scatter:
    def __init__(self, order):
        self.order = order

    def odd(self, fn, *xs):
        self.recv = swap(self.order.step(lambda *t: fn(*t).astype(BF16), *xs), 1)

    def even(self, fn, *xs):
        self.q = self.order.step(lambda r, *t: (fn(*t) + r.astype(F32)).astype(BF16), self.recv, *xs)

    def send(self):
        (q,) = self.order.tie(self.q)
        n = q.shape[0] // 4
        half = n // 2
        q0a, q0b, q2a, q2b, q4a, q4b, q6a, q6b = (q[i * half:(i + 1) * half] for i in range(8))
        self.r4a, self.r2b = swap(q6a, 2), swap(q6b, 4)
        self.a2, self.b4 = swap(q2a, 2), swap(q4b, 4)
        self.keep = (q0a, q0b)
        self.mids = (q2b, q4a)

    def mid(self):
        def add(q2b, r2b, q4a, r4a):
            return (q2b.astype(F32) + r2b.astype(F32)).astype(BF16), (q4a.astype(F32) + r4a.astype(F32)).astype(BF16)

        b2, a4 = self.order.step(add, self.mids[0], self.r2b, self.mids[1], self.r4a)
        self.b2, self.a4 = swap(b2, 2), swap(a4, 4)

    def final(self, fn, *xs):
        def add(q0a, q0b, a2, b2, a4, b4, *t):
            top = q0a.astype(F32) + a2.astype(F32) + a4.astype(F32)
            bottom = q0b.astype(F32) + b2.astype(F32) + b4.astype(F32)
            return fn(jnp.concatenate([top, bottom], axis=0), *t)

        return self.order.step(add, *self.keep, self.a2, self.b2, self.a4, self.b4, *xs)


def butterfly_sum(x):
    for mask in (1, 2, 4):
        x = x + swap(x, mask)
    return x


def dot(a, b):
    return lax.dot_general(a, b, (((1,), (0,)), ((), ())), preferred_element_type=F32)


def dot_t(a, b):
    return lax.dot_general(a, b, (((1,), (1,)), ((), ())), preferred_element_type=F32)


def dot_w(a, b):
    return lax.dot_general(a, b, (((0,), (0,)), ((), ())), preferred_element_type=F32)


def inv_rms(x_f):
    return lax.rsqrt(jnp.mean(x_f * x_f, axis=-1, keepdims=True) + NORM_EPS)


def rms_norm(x, gain):
    x_f = x.astype(F32)
    return (x_f * inv_rms(x_f) * gain).astype(BF16)


def rms_pull(x, gain, dy):
    x_f, dy = x.astype(F32), dy.astype(BF16).astype(F32)
    r = inv_rms(x_f)
    unit = x_f * r
    scaled = dy * gain
    dx = r * (scaled - unit * jnp.mean(scaled * unit, axis=-1, keepdims=True))
    return dx, jnp.sum(dy * unit, axis=0)


def gated_act(gate, upper):
    return (jax.nn.gelu(gate, approximate=True) * upper).astype(BF16)


def rope_tables(positions, head_dim):
    half_dim = head_dim // 2
    exponent = jnp.arange(half_dim, dtype=F32) * (2.0 / head_dim)
    inv_freq = jnp.exp(exponent * (-math.log(10000.0)))
    angles = positions.astype(F32)[..., None] * inv_freq
    return jnp.cos(angles), jnp.sin(angles)


def rotate(x, cos_t, sin_t):
    half = x.shape[-1] // 2
    first, second = x[:, :half], x[:, half:]
    return jnp.concatenate([first * cos_t - second * sin_t, second * cos_t + first * sin_t], axis=-1)


def unrotate(x, cos_t, sin_t):
    half = x.shape[-1] // 2
    first, second = x[:, :half], x[:, half:]
    return jnp.concatenate([first * cos_t + second * sin_t, second * cos_t - first * sin_t], axis=-1)


def flat(ref):
    x = ref[...]
    return x.reshape(-1, x.shape[-1])


def softmax_rows(q, k, q_pos, k_pos, prefix, valid):
    s = dot_t(q, k) * (q.shape[-1] ** -0.5)
    visible = (k_pos < valid) & ((k_pos < prefix) | (k_pos <= q_pos))
    s = jnp.where(visible, s, -1e30)
    e = jnp.exp(s - jnp.max(s, axis=-1, keepdims=True))
    return e * (1.0 / jnp.sum(e, axis=-1, keepdims=True))


def attn_fwd_kernel(first_seq, pre_ref, val_ref, qe, qo, ke, ko, ve, vo, cos_e, sin_e, cos_o, sin_o, qpos_ref, kpos_ref, ae, ao):
    seq = first_seq + pl.program_id(0)
    prefix, valid = pre_ref[seq], val_ref[seq]
    ce, se, co, so = flat(cos_e), flat(sin_e), flat(cos_o), flat(sin_o)
    k = jnp.concatenate([rotate(flat(ke), ce, se).astype(BF16), rotate(flat(ko), co, so).astype(BF16)], axis=0)
    v = jnp.concatenate([flat(ve), flat(vo)], axis=0).astype(BF16)
    k_pos = kpos_ref[...]
    rows = ce.shape[0]
    for i, (q_ref, c, s, a_ref) in enumerate(((qe, ce, se, ae), (qo, co, so, ao))):
        q = rotate(flat(q_ref), c, s).astype(BF16)
        p = softmax_rows(q, k, qpos_ref[i * rows:(i + 1) * rows, :], k_pos, prefix, valid)
        a_ref[...] = dot(p.astype(BF16), v).astype(BF16).reshape(a_ref.shape)


def attn_bwd_kernel(first_seq, pre_ref, val_ref, qe, qo, ke, ko, ve, vo, cos_e, sin_e, cos_o, sin_o, qpos_ref, kpos_ref, dae, dao,
                    dqe, dqo, dkve, dkvo, dk_acc, dv_acc):
    head = pl.program_id(1)
    seq = first_seq + pl.program_id(0)
    prefix, valid = pre_ref[seq], val_ref[seq]
    ce, se, co, so = flat(cos_e), flat(sin_e), flat(cos_o), flat(sin_o)
    k = jnp.concatenate([rotate(flat(ke), ce, se).astype(BF16), rotate(flat(ko), co, so).astype(BF16)], axis=0)
    v = jnp.concatenate([flat(ve), flat(vo)], axis=0).astype(BF16)
    k_pos = kpos_ref[...]
    rows = ce.shape[0]
    scale = k.shape[-1] ** -0.5

    @pl.when(head == 0)
    def _():
        dk_acc[...] = jnp.zeros_like(dk_acc)
        dv_acc[...] = jnp.zeros_like(dv_acc)

    for i, (q_ref, c, s, da_ref, dq_ref) in enumerate(((qe, ce, se, dae, dqe), (qo, co, so, dao, dqo))):
        q = rotate(flat(q_ref), c, s).astype(BF16)
        p = softmax_rows(q, k, qpos_ref[i * rows:(i + 1) * rows, :], k_pos, prefix, valid)
        da = flat(da_ref)
        dv_acc[...] += dot_w(p.astype(BF16), da)
        dp = dot_t(da, v)
        ds = (p * (dp - jnp.sum(p * dp, axis=-1, keepdims=True))).astype(BF16)
        dq_ref[...] = unrotate(dot(ds, k) * scale, c, s).astype(BF16).reshape(dq_ref.shape)
        dk_acc[...] += dot_w(ds, q) * scale

    @pl.when(head == pl.num_programs(1) - 1)
    def _():
        dk, dv = dk_acc[...], dv_acc[...]
        dim = dk.shape[-1]
        for out, lo, c, s in ((dkve, 0, ce, se), (dkvo, rows, co, so)):
            part = jnp.concatenate([unrotate(dk[lo:lo + rows], c, s), dv[lo:lo + rows]], axis=-1)
            out[...] = part.astype(BF16).reshape(out.shape)


def attention_call(backward, first_seq, lens, qkv_e, qkv_o, tables, q_pos, k_pos, heads, grads=()):
    slots, seqs, toks, _ = qkv_e.shape
    dim = tables[0].shape[-1] * 2

    def block(width, col):
        return pl.BlockSpec((slots, None, toks, width), lambda i, h, *_: (0, i, 0, col(h)))

    q_spec = block(dim, lambda h: h)
    k_spec = block(dim, lambda h: heads)
    v_spec = block(dim, lambda h: heads + 1)
    table_spec = pl.BlockSpec((slots, toks, dim // 2), lambda i, h, *_: (0, 0, 0))
    in_specs = [q_spec, q_spec, k_spec, k_spec, v_spec, v_spec] + [table_spec] * 4
    in_specs += [pl.BlockSpec(q_pos.shape, lambda i, h, *_: (0, 0)), pl.BlockSpec(k_pos.shape, lambda i, h, *_: (0, 0))]
    a_shape = jax.ShapeDtypeStruct((slots, seqs, toks, heads * dim), BF16)
    out_shape, out_specs, scratch = [a_shape, a_shape], [q_spec, q_spec], []
    body = attn_fwd_kernel
    flops = 4 * seqs * heads * dim * (2 * slots * toks) ** 2
    if backward:
        body = attn_bwd_kernel
        flops = flops * 5 // 2
        in_specs += [q_spec, q_spec]
        kv_shape = jax.ShapeDtypeStruct((slots, seqs, toks, 2 * dim), BF16)
        kv_spec = block(2 * dim, lambda h: 0)
        out_shape += [kv_shape, kv_shape]
        out_specs += [kv_spec, kv_spec]
        scratch = [pltpu.VMEM((2 * slots * toks, dim), F32)] * 2
    return pl.pallas_call(
        functools.partial(body, first_seq),
        grid_spec=pltpu.PrefetchScalarGridSpec(num_scalar_prefetch=2, grid=(seqs, heads), in_specs=in_specs, out_specs=out_specs, scratch_shapes=scratch),
        out_shape=out_shape,
        compiler_params=pltpu.CompilerParams(dimension_semantics=("arbitrary", "arbitrary")),
        cost_estimate=pl.CostEstimate(flops=flops * 4, bytes_accessed=seqs * heads * 8 * 2 ** 20, transcendentals=seqs * heads * (2 * slots * toks) ** 2),
    )(*lens, qkv_e, qkv_o, qkv_e, qkv_o, qkv_e, qkv_o, *tables, q_pos, k_pos, *grads)


def solution(mesh):
    act_spec = P("dp", "tp", None)
    in_specs = (act_spec, act_spec, P("dp"), P("dp"), P(None), P(None, "tp"), P(None, None), P(None, None), P("tp", None), P(None), P(None, "tp"), P(None, "tp"), P("tp", None))
    out_specs = (act_spec, act_spec, P("dp"), P("dp", "tp"), P("dp", None), P("dp", None), P(("dp", "tp"), None), P("dp"), P("dp", "tp"), P("dp", "tp"), P(("dp", "tp"), None))

    def local_layer(hidden, grad_out, prefix_len, valid_len, attn_norm, w_query, w_key, w_value, w_out, mlp_norm, w_gate, w_up, w_down):
        batch, toks, width = hidden.shape
        dim = w_key.shape[1]
        heads = w_query.shape[1] // dim
        seqs = batch // NUM_CHUNKS
        n = seqs * toks
        me = lax.axis_index("tp")
        slot_even = me ^ (2 * jnp.arange(4))
        pos_even = slot_even[:, None] * toks + jnp.arange(toks)
        pos_odd = (slot_even ^ 1)[:, None] * toks + jnp.arange(toks)
        tables = rope_tables(pos_even, dim) + rope_tables(pos_odd, dim)
        pos_all = jnp.concatenate([pos_even.reshape(-1), pos_odd.reshape(-1)])
        q_pos, k_pos = pos_all[:, None], pos_all[None, :]
        lens = (prefix_len, valid_len)
        gain1 = 1.0 + attn_norm.astype(F32)
        gain2 = 1.0 + mlp_norm.astype(F32)
        order = Order()
        step = order.step
        chunks = range(NUM_CHUNKS)

        def rows_of(x, c):
            return x[c * seqs:(c + 1) * seqs].reshape(n, width)

        def slots4(x):
            return x.reshape(4, seqs, toks, x.shape[-1])

        def rows2(x):
            return x.reshape(-1, x.shape[-1])

        def scatters():
            return [Scatter(order) for _ in chunks]

        hid = [rows_of(hidden, c) for c in chunks]
        gout = [rows_of(grad_out, c) for c in chunks]
        rs_attn, rs_mlp, rs_dz, rs_du, rs_dkv = (scatters() for _ in range(5))
        normed = [rms_norm(hid[c], gain1) for c in chunks]
        u_all, qkv, mixed, resid, gated_in, z_all, g_all = ([None] * NUM_CHUNKS for _ in range(7))
        saved = [[None, None] for _ in chunks]
        act, d_gate, d_up = ([[None, None] for _ in chunks] for _ in range(3))
        d_h1, g_mlp_part, dh_all, dq_all, dkv_out, hidden_out = ([None] * NUM_CHUNKS for _ in range(6))

        def project(c, i):
            qkv[c] = (qkv[c] or []) + [slots4(step(dot, u_all[c][i], w_qkv))]

        def attend(c):
            def run(q_e, q_o):
                return [rows2(a) for a in attention_call(False, c * seqs, lens, q_e, q_o, tables, q_pos, k_pos, heads)]

            mixed[c] = step(run, *qkv[c])

        def post_attention(c):
            def run(total, h):
                h1 = (h.astype(F32) + total).astype(BF16)
                return rms_norm(h1, gain2), h1

            gated_in[c], resid[c] = rs_attn[c].final(run, hid[c])

        def gate_proj(c, i):
            saved[c][i] = step(dot, z_all[c][i], w_gate)

        def up_proj(c, i):
            def run(gate, z, w):
                up = dot(z, w)
                return gated_act(gate, up), up

            act[c][i], up = step(run, saved[c][i], z_all[c][i], w_up)
            saved[c][i] = (saved[c][i], up)

        def act_grad(c, i):
            def run(g, w, gate, up):
                d_a = dot_t(g, w).astype(BF16)
                dg, du = jax.vjp(gated_act, gate, up)[1](d_a)
                return dg.astype(BF16), du.astype(BF16)

            d_gate[c][i], d_up[c][i] = step(run, g_all[c][i], w_down, *saved[c][i])

        def dz_part(dg, du, wg, wu):
            return dot_t(dg, wg) + dot_t(du, wu)

        def mlp_out(total, h):
            return (h.astype(F32) + total).astype(BF16)

        def post_dz(c):
            def run(total, h1, g):
                dx, g_part = rms_pull(h1, gain2, total)
                return (g.astype(F32) + dx.astype(BF16).astype(F32)).astype(BF16), g_part

            d_h1[c], g_mlp_part[c] = rs_dz[c].final(run, resid[c], gout[c])

        def attend_grad(c):
            def run(d_e, d_o, w, q_e, q_o):
                dmix = [slots4(dot_t(d, w).astype(BF16)) for d in (d_e, d_o)]
                return [rows2(x) for x in attention_call(True, c * seqs, lens, q_e, q_o, tables, q_pos, k_pos, heads, dmix)]

            dq_e, dq_o, dkv_e, dkv_o = step(run, *dh_all[c], w_out, *qkv[c])
            dq_all[c] = (dq_e, dq_o)
            rs_dkv[c].odd(lambda x: x, dkv_o)
            rs_du[c].odd(dot_t, dq_o, w_query)
            rs_du[c].even(dot_t, dq_e, w_query)
            rs_dkv[c].even(lambda x: x.astype(F32), dkv_e)

        class WeightGrad:
            def __init__(self, lefts, rights):
                self.pairs = [(lefts, rights, c, i) for c in chunks for i in range(2)]
                self.total = None

            def add(self, count=1):
                for _ in range(count):
                    lefts, rights, c, i = self.pairs.pop(0)
                    if self.total is None:
                        self.total = step(dot_w, lefts[c][i], rights[c][i])
                    else:
                        self.total = step(lambda t, a, b: t + dot_w(a, b), self.total, lefts[c][i], rights[c][i])

        wg_down, wg_gate, wg_up = WeightGrad(act, g_all), WeightGrad(z_all, d_gate), WeightGrad(z_all, d_up)
        wg_out, wg_query = WeightGrad(mixed, dh_all), WeightGrad(u_all, dq_all)

        ag_u0 = Gather(order, normed[0])
        w_qkv = step(lambda *w: jnp.concatenate(w, axis=1), w_query, w_key, w_value)
        ag_u0.forward()
        ag_u1 = Gather(order, normed[1])
        u_all[0] = ag_u0.finish()
        project(0, 0)
        project(0, 1)
        ag_u1.forward()
        attend(0)
        rs_attn[0].odd(dot, mixed[0][1], w_out)
        rs_attn[0].even(dot, mixed[0][0], w_out)
        rs_attn[0].send()
        u_all[1] = ag_u1.finish()
        project(1, 0)
        project(1, 1)
        rs_attn[0].mid()
        attend(1)
        rs_attn[1].odd(dot, mixed[1][1], w_out)
        rs_attn[1].even(dot, mixed[1][0], w_out)
        post_attention(0)
        ag_z0 = Gather(order, gated_in[0])
        ag_z0.forward()
        rs_attn[1].send()
        z_all[0] = ag_z0.finish()
        gate_proj(0, 0)
        rs_attn[1].mid()
        up_proj(0, 0)
        gate_proj(0, 1)
        post_attention(1)
        ag_z1 = Gather(order, gated_in[1])
        up_proj(0, 1)
        ag_z1.forward()
        ag_g0 = Gather(order, gout[0])
        rs_mlp[0].odd(dot, act[0][1], w_down)
        rs_mlp[0].even(dot, act[0][0], w_down)
        z_all[1] = ag_z1.finish()
        gate_proj(1, 0)
        ag_g0.forward()
        ag_g1 = Gather(order, gout[1])
        up_proj(1, 0)
        gate_proj(1, 1)
        g_all[0] = ag_g0.finish()
        up_proj(1, 1)
        ag_g1.forward()
        rs_mlp[0].send()
        act_grad(0, 0)
        act_grad(0, 1)
        g_all[1] = ag_g1.finish()
        rs_dz[0].odd(dz_part, d_gate[0][1], d_up[0][1], w_gate, w_up)
        rs_mlp[0].mid()
        act_grad(1, 0)
        rs_dz[0].even(dz_part, d_gate[0][0], d_up[0][0], w_gate, w_up)
        rs_dz[0].send()
        hidden_out[0] = rs_mlp[0].final(mlp_out, resid[0])
        act_grad(1, 1)
        rs_dz[0].mid()
        rs_dz[1].odd(dz_part, d_gate[1][1], d_up[1][1], w_gate, w_up)
        rs_mlp[1].odd(dot, act[1][1], w_down)
        post_dz(0)
        ag_d0 = Gather(order, d_h1[0])
        rs_dz[1].even(dz_part, d_gate[1][0], d_up[1][0], w_gate, w_up)
        ag_d0.forward()
        rs_dz[1].send()
        rs_mlp[1].even(dot, act[1][0], w_down)
        wg_down.add()
        rs_dz[1].mid()
        dh_all[0] = ag_d0.finish()
        attend_grad(0)
        wg_down.add()
        post_dz(1)
        ag_d1 = Gather(order, d_h1[1])
        wg_down.add()
        ag_d1.forward()
        rs_dkv[0].send()
        rs_du[0].send()
        wg_down.add()
        rs_dkv[0].mid()
        rs_du[0].mid()
        wg_gate.add()
        dh_all[1] = ag_d1.finish()
        attend_grad(1)
        rs_dkv[1].send()
        rs_du[1].send()
        wg_gate.add()
        rs_dkv[1].mid()
        rs_du[1].mid()
        rs_mlp[1].send()
        wg_gate.add(2)

        def post_du(c):
            d_kv = rs_dkv[c].final(lambda t: t.astype(BF16))

            def run(total, x, d_h, kv, wk, wv):
                d_u = total + dot_t(kv[:, :dim], wk) + dot_t(kv[:, dim:], wv)
                dx, g_part = rms_pull(x, gain1, d_u)
                return (d_h.astype(F32) + dx.astype(BF16).astype(F32)).astype(BF16), g_part

            out, g_part = rs_du[c].final(run, hid[c], d_h1[c], d_kv, w_key, w_value)
            return d_kv, out, g_part

        d_kv0, grad_hidden0, g_attn0 = post_du(0)
        rs_mlp[1].mid()
        wg_up.add()
        d_kv1, grad_hidden1, g_attn1 = post_du(1)

        def kv_grad(lo):
            return lambda u0, k0, u1, k1: dot_w(u0, k0[:, lo:lo + dim]) + dot_w(u1, k1[:, lo:lo + dim])

        g_key = step(kv_grad(0), normed[0], d_kv0, normed[1], d_kv1)
        g_value = step(kv_grad(dim), normed[0], d_kv0, normed[1], d_kv1)
        g_key, g_value = lax.psum((g_key, g_value), "tp")
        wg_up.add()
        hidden_out[1] = rs_mlp[1].final(mlp_out, resid[1])
        g_norms = butterfly_sum(jnp.stack([g_attn0 + g_attn1, g_mlp_part[0] + g_mlp_part[1]]))
        wg_up.add(2)
        wg_out.add(4)
        wg_query.add(4)

        def join(parts):
            return jnp.concatenate(parts, axis=0).reshape(batch, toks, width)

        return (join(hidden_out), join([grad_hidden0, grad_hidden1]), g_norms[0], wg_query.total, g_key, g_value, wg_out.total, g_norms[1], wg_gate.total, wg_up.total, wg_down.total)

    return jax.shard_map(local_layer, mesh=mesh, in_specs=in_specs, out_specs=out_specs, check_vma=False)
```
